8 devices in a mesh: rep: 1 (over z), dp: 8 (over x, y, core).
Axes of the slice: x: 2, y: 2, z: 1, core: 2. Of those that a mesh axis runs over, the one named last changes fastest.
Arguments:
- a: bfloat16 [8, 4, 4096, 1024], P(('rep', 'dp'))
- g: bfloat16 [8, 4, 4096, 4096], P(('rep', 'dp'))
Outputs:
- output: bfloat16 [4, 1024, 4096], P('rep')
All inputs are finite; a program needn't handle non-finite values.
Results may differ from the reference program's by a relative error of at most 0.012.
Values are sent between devices in bfloat16 or wider.
A program may use at most 2 GiB of HBM per device.

```python
import jax
import jax.numpy as jnp
from jax import lax

DEVICES = 8
MATRICES = 4
TOKENS = 4096
D = 1024
FF = 4096


def setup_inputs(seed: int = 0, part: int = 0) -> dict:
    ka, kg, ks = (jax.random.fold_in(k, part) for k in jax.random.split(jax.random.key(seed), 3))
    size = 2.0 ** jax.random.uniform(ks, (DEVICES, MATRICES, 1, 1), jnp.float32, -1.0, 1.0)
    a = jax.random.normal(ka, (DEVICES, MATRICES, TOKENS, D), jnp.float32)
    g = size * jax.random.normal(kg, (DEVICES, MATRICES, TOKENS, FF), jnp.float32) * (DEVICES * TOKENS) ** -0.5
    return {"a": a.astype(jnp.bfloat16), "g": g.astype(jnp.bfloat16)}


def reference(a, g):
    def take(so_far, one):
        return so_far + jnp.einsum("ntd,ntf->ndf", *one, preferred_element_type=jnp.float32), None

    return lax.scan(take, jnp.zeros((MATRICES, D, FF), jnp.float32), (a, g))[0].astype(jnp.bfloat16)
```

```python
import functools

import jax
import jax.numpy as jnp
from jax import lax
from jax.experimental import pallas as pl
from jax.experimental.pallas import tpu as pltpu
from jax.sharding import PartitionSpec as P

MESH = pl.DeviceIdType.MESH
LAG = 2
SLOTS = 4


def flip(i, bit):
    return i + bit - 2 * bit * ((i // bit) % 2)


def kernel(
    cfg, a_ref, g_ref, o_ref,
    a_raw, a_t, g_buf, d2d_out, d2d_in, part, keep1, rs1_out, rs1_in, keep2, rs2_out, rs2_in, done,
    a_sem, g_sem, d2d_s, d2d_r, rs1_s, rs1_r, rs2_s, rs2_r, loc_s, ag1_s, ag1_r, ag2_s, ag2_r, ag3_s, ag3_r,
):
    mats, tokens, d, ff, width, blocks = cfg
    per = ff // width
    steps = mats * per
    half, quarter, eighth = d // 2, d // 4, d // 8
    rows_a = tokens // blocks

    me = lax.axis_index("dp")
    core, y, x = me % 2, (me // 2) % 2, (me // 4) % 2
    cu = x + core * (y - x)
    cv = y + core * (x - y)
    mate = flip(me, 1)
    at_x, at_y = flip(me, 4), flip(me, 2)
    u = at_x + core * (at_y - at_x)
    v = at_y + core * (at_x - at_y)

    mine = pl.multiple_of(core * half, half)
    theirs = pl.multiple_of((1 - core) * half, half)
    q_keep = pl.multiple_of(cu * quarter, quarter)
    q_send = pl.multiple_of((1 - cu) * quarter, quarter)
    e_keep = pl.multiple_of(cv * eighth, eighth)
    e_send = pl.multiple_of((1 - cv) * eighth, eighth)

    def remote(src, dst, s_sem, r_sem, to):
        return pltpu.make_async_remote_copy(
            src_ref=src, dst_ref=dst, send_sem=s_sem, recv_sem=r_sem, device_id={"dp": to}, device_id_type=MESH
        )

    def g_copy(s):
        n, j = s // per, s % per
        cols = pl.ds(pl.multiple_of(j * width, width), width)
        return pltpu.make_async_copy(g_ref.at[0, n, :, cols], g_buf.at[s % 2], g_sem.at[s % 2])

    def a_copy(b):
        n, t = b // blocks, b % blocks
        rows = pl.ds(pl.multiple_of(t * rows_a, rows_a), rows_a)
        return pltpu.make_async_copy(a_ref.at[0, n, rows, :], a_raw.at[b % 2], a_sem.at[b % 2])

    def turn(b):
        a_copy(b).wait()
        n, t = b // blocks, b % blocks
        cols = pl.ds(pl.multiple_of(t * rows_a, rows_a), rows_a)
        a_t[n % 2, :, cols] = a_raw[b % 2].T

        @pl.when(b + 2 < mats * blocks)
        def _():
            a_copy(b + 2).start()

    def region(k, start, rows):
        n, j = k // per, k % per
        return o_ref.at[n, pl.ds(start, rows), pl.ds(pl.multiple_of(j * width, width), width)]

    def d2d(s):
        return remote(d2d_out, d2d_in.at[s % 2], d2d_s.at[0], d2d_r.at[s % 2], mate)

    def rs1(k):
        i = k % SLOTS
        return remote(rs1_out.at[i], rs1_in.at[i], rs1_s.at[i], rs1_r.at[i], u)

    def rs2(k):
        i = k % SLOTS
        return remote(rs2_out.at[i], rs2_in.at[i], rs2_s.at[i], rs2_r.at[i], v)

    e_row = pl.multiple_of(mine + q_keep + e_keep, eighth)
    q_row = pl.multiple_of(mine + q_keep, quarter)

    def local(k):
        i = k % SLOTS
        return pltpu.make_async_copy(done.at[i], region(k, e_row, eighth), loc_s.at[i])

    def ag1(k):
        i = k % SLOTS
        return remote(done.at[i], region(k, e_row, eighth), ag1_s.at[i], ag1_r.at[i], v)

    def ag2(k):
        i = k % SLOTS
        r = region(k, q_row, quarter)
        return remote(r, r, ag2_s.at[i], ag2_r.at[i], u)

    def ag3(k):
        i = k % SLOTS
        r = region(k, mine, half)
        return remote(r, r, ag3_s.at[i], ag3_r.at[i], mate)

    def events(s):
        def on(lag, f):
            k = s - lag
            pl.when(jnp.logical_and(k >= 0, k < steps))(lambda: f(k))

        @functools.partial(on, 5 * LAG)
        def _(k):
            ag3(k).wait()

        @functools.partial(on, 4 * LAG)
        def _(k):
            ag2(k).wait()
            ag3(k).start()

        @functools.partial(on, 3 * LAG)
        def _(k):
            local(k).wait()
            ag1(k).wait()
            ag2(k).start()

        @functools.partial(on, 2 * LAG)
        def _(k):
            rs2(k).wait()
            i = k % SLOTS
            done[i] = (keep2[i] + rs2_in[i].astype(jnp.float32)).astype(jnp.bfloat16)
            ag1(k).start()
            local(k).start()

        @functools.partial(on, LAG)
        def _(k):
            rs1(k).wait()
            i = k % SLOTS
            rows = pl.ds(e_send, eighth)
            rs2_out[i] = (keep1[i, rows, :] + rs1_in[i, rows, :].astype(jnp.float32)).astype(jnp.bfloat16)
            rs2(k).start()
            rows = pl.ds(e_keep, eighth)
            keep2[i] = keep1[i, rows, :] + rs1_in[i, rows, :].astype(jnp.float32)

    a_copy(0).start()
    a_copy(1).start()
    g_copy(0).start()

    barrier = pltpu.get_barrier_semaphore()
    for other in (mate, u, v):
        pl.semaphore_signal(barrier, inc=1, device_id={"dp": other}, device_id_type=MESH)
    pl.semaphore_wait(barrier, 3)

    @pl.loop(0, blocks)
    def _(b):
        turn(b)

    @pl.loop(0, steps)
    def _(s):
        n, j = s // per, s % per
        g_copy(s).wait()

        @pl.when(s + 1 < steps)
        def _():
            g_copy(s + 1).start()

        d2d_out[...] = jnp.dot(
            a_t[n % 2, pl.ds(theirs, half), :], g_buf[s % 2], preferred_element_type=jnp.float32
        ).astype(jnp.bfloat16)
        d2d(s).start()
        events(s)
        part[...] = jnp.dot(a_t[n % 2, pl.ds(mine, half), :], g_buf[s % 2], preferred_element_type=jnp.float32)

        @pl.when(n + 1 < mats)
        def _():
            turn((n + 1) * blocks + j)

        d2d(s).wait()
        i, h = s % SLOTS, s % 2
        rows = pl.ds(q_send, quarter)
        rs1_out[i] = (part[rows, :] + d2d_in[h, rows, :].astype(jnp.float32)).astype(jnp.bfloat16)
        rs1(s).start()
        rows = pl.ds(q_keep, quarter)
        keep1[i] = part[rows, :] + d2d_in[h, rows, :].astype(jnp.float32)

    @pl.loop(steps, steps + 5 * LAG)
    def _(s):
        events(s)


def solution(mesh):
    def step(a, g):
        _, mats, tokens, d = a.shape
        ff = g.shape[-1]
        width = 512 if ff % 512 == 0 else ff
        blocks = ff // width
        half, quarter, eighth = d // 2, d // 4, d // 8
        f32, bf16 = jnp.float32, jnp.bfloat16
        dma = pltpu.SemaphoreType.DMA
        return pl.pallas_call(
            functools.partial(kernel, (mats, tokens, d, ff, width, blocks)),
            out_shape=jax.ShapeDtypeStruct((mats, d, ff), bf16),
            in_specs=[pl.BlockSpec(memory_space=pl.ANY)] * 2,
            out_specs=pl.BlockSpec(memory_space=pl.ANY),
            scratch_shapes=[
                pltpu.VMEM((2, tokens // blocks, d), bf16),
                pltpu.VMEM((2, d, tokens), bf16),
                pltpu.VMEM((2, tokens, width), bf16),
                pltpu.VMEM((half, width), bf16),
                pltpu.VMEM((2, half, width), bf16),
                pltpu.VMEM((half, width), f32),
                pltpu.VMEM((SLOTS, quarter, width), f32),
                pltpu.VMEM((SLOTS, quarter, width), bf16),
                pltpu.VMEM((SLOTS, quarter, width), bf16),
                pltpu.VMEM((SLOTS, eighth, width), f32),
                pltpu.VMEM((SLOTS, eighth, width), bf16),
                pltpu.VMEM((SLOTS, eighth, width), bf16),
                pltpu.VMEM((SLOTS, eighth, width), bf16),
                dma((2,)), dma((2,)), dma((1,)), dma((2,)),
                dma((SLOTS,)), dma((SLOTS,)), dma((SLOTS,)), dma((SLOTS,)), dma((SLOTS,)),
                dma((SLOTS,)), dma((SLOTS,)), dma((SLOTS,)), dma((SLOTS,)), dma((SLOTS,)), dma((SLOTS,)),
            ],
            compiler_params=pltpu.CompilerParams(
                collective_id=0, has_side_effects=True, vmem_limit_bytes=60 * 2**20
            ),
        )(a, g)

    spec = P(("rep", "dp"), None, None, None)
    return jax.shard_map(step, mesh=mesh, in_specs=(spec, spec), out_specs=P("rep", None, None), check_vma=False)
```

```python
import functools

import jax
import jax.numpy as jnp
from jax import lax
from jax.experimental import pallas as pl
from jax.experimental.pallas import tpu as pltpu
from jax.sharding import PartitionSpec as P

MESH = pl.DeviceIdType.MESH
SLOTS = 4
HELD = 8
RAW = 4
RS1, RS2, AG1, AG2, AG3 = 1, 2, 3, 5, 6


def flip(i, bit):
    return i + bit - 2 * bit * ((i // bit) % 2)


def kernel(
    cfg, a_ref, g_ref, o_ref,
    a_raw, a_t, g_buf, d2d_out, d2d_in, part, keep1, rs1_out, rs1_in, keep2, rs2_out, rs2_in,
    a_sem, g_sem, g0_sem, d2d_s, d2d_r, rs1_s, rs1_r, rs2_s, rs2_r, ag1_s, ag1_r, ag2_s, ag2_r, ag3_s, ag3_r,
):
    mats, tokens, d, ff, width, blocks = cfg
    per = ff // width
    steps = mats * per
    half, quarter, eighth = d // 2, d // 4, d // 8
    rows_a = tokens // blocks
    f32, bf16 = jnp.float32, jnp.bfloat16

    me = lax.axis_index("dp")
    core, y, x = me % 2, (me // 2) % 2, (me // 4) % 2
    cu = x + core * (y - x)
    cv = y + core * (x - y)
    mate = flip(me, 1)
    at_x, at_y = flip(me, 4), flip(me, 2)
    u = at_x + core * (at_y - at_x)
    v = at_y + core * (at_x - at_y)

    mine = pl.multiple_of(core * half, half)
    theirs = pl.multiple_of((1 - core) * half, half)
    q_keep = pl.ds(pl.multiple_of(cu * quarter, quarter), quarter)
    q_send = pl.ds(pl.multiple_of((1 - cu) * quarter, quarter), quarter)
    e_keep = pl.ds(pl.multiple_of(cv * eighth, eighth), eighth)
    e_send = pl.ds(pl.multiple_of((1 - cv) * eighth, eighth), eighth)
    rows_h = pl.ds(mine, half)
    rows_send = pl.ds(pl.multiple_of(mine + (1 - cu) * quarter, quarter), quarter)
    rows_q = pl.ds(pl.multiple_of(mine + cu * quarter, quarter), quarter)
    rows_e = pl.ds(pl.multiple_of(mine + cu * quarter + cv * eighth, eighth), eighth)

    def remote(src, dst, s_sem, r_sem, to):
        return pltpu.make_async_remote_copy(
            src_ref=src, dst_ref=dst, send_sem=s_sem, recv_sem=r_sem, device_id={"dp": to}, device_id_type=MESH
        )

    part_w = width // 2

    def cols(k):
        return pl.ds(pl.multiple_of((k % per) * width, width), width)

    def cols_of(k, p):
        return pl.ds(pl.multiple_of((k % per) * width + p * part_w, part_w), part_w)

    def lanes(p):
        return pl.ds(p * part_w, part_w)

    def g_copy(s):
        return pltpu.make_async_copy(g_ref.at[0, s // per, :, cols(s)], g_buf.at[s % 2], g_sem.at[s % 2])

    def g_first(b):
        rows = pl.ds(b * rows_a, rows_a)
        return pltpu.make_async_copy(g_ref.at[0, 0, rows, pl.ds(0, width)], g_buf.at[0, rows, :], g0_sem.at[b])

    def a_copy(b):
        rows = pl.ds(pl.multiple_of((b % blocks) * rows_a, rows_a), rows_a)
        return pltpu.make_async_copy(a_ref.at[0, b // blocks, rows, :], a_raw.at[b % RAW], a_sem.at[b % RAW])

    def d2d(s):
        return remote(d2d_out, d2d_in.at[s % 2], d2d_s.at[0], d2d_r.at[s % 2], mate)

    def rs1(k, p):
        i, j = k % SLOTS, k % SLOTS * 2 + p
        return remote(rs1_out.at[i, :, lanes(p)], rs1_in.at[i, :, lanes(p)], rs1_s.at[j], rs1_r.at[j], u)

    def rs2(k, p):
        i, j = k % SLOTS, k % SLOTS * 2 + p
        return remote(rs2_out.at[i, :, lanes(p)], rs2_in.at[i, :, lanes(p)], rs2_s.at[j], rs2_r.at[j], v)

    def gather(k, p, rows, s_sem, r_sem, to):
        j = k % HELD * 2 + p
        r = o_ref.at[k // per, rows, cols_of(k, p)]
        return remote(r, r, s_sem.at[j], r_sem.at[j], to)

    def ag1(k, p):
        return gather(k, p, rows_e, ag1_s, ag1_r, v)

    def ag2(k, p):
        return gather(k, p, rows_q, ag2_s, ag2_r, u)

    def ag3(k, p):
        return gather(k, p, rows_h, ag3_s, ag3_r, mate)

    def at(s, lag):
        def run(f):
            k = s - lag
            pl.when(jnp.logical_and(k >= 0, k < steps))(lambda: f(k))
        return run

    def events(s, p):
        c = lanes(p)

        @at(s, AG3)
        def _(k):
            ag3(k, p).wait()

        @at(s, AG2)
        def _(k):
            ag2(k, p).wait()
            ag3(k, p).start()

        @at(s, AG1)
        def _(k):
            ag1(k, p).wait()
            ag2(k, p).start()

        @at(s, RS2)
        def _(k):
            rs2(k, p).wait()
            i = k % SLOTS
            o_ref[k // per, rows_e, cols_of(k, p)] = (keep2[i, :, c] + rs2_in[i, :, c].astype(f32)).astype(bf16)
            ag1(k, p).start()

        @at(s, RS1)
        def _(k):
            rs1(k, p).wait()
            i = k % SLOTS
            rs2_out[i, :, c] = (keep1[i, e_send, c] + rs1_in[i, e_send, c].astype(f32)).astype(bf16)
            rs2(k, p).start()
            keep2[i, :, c] = keep1[i, e_keep, c] + rs1_in[i, e_keep, c].astype(f32)

    def pair(s):
        d2d(s).wait()
        i, h = s % SLOTS, s % 2
        for p in range(2):
            c = lanes(p)
            rs1_out[i, :, c] = (part[rows_send, c] + d2d_in[h, q_send, c].astype(f32)).astype(bf16)
            rs1(s, p).start()
        keep1[i] = part[rows_q, :] + d2d_in[h, q_keep, :].astype(f32)

    def dot(rows, s):
        return jnp.dot(a_t[pl.ds(rows, half), :], g_buf[s % 2], preferred_element_type=f32)

    for b in range(RAW):
        a_copy(b).start()
        g_first(b).start()

    barrier = pltpu.get_barrier_semaphore()
    for peer in (mate, u, v):
        pl.semaphore_signal(barrier, inc=1, device_id={"dp": peer}, device_id_type=MESH)

    for b in range(blocks + 1):
        if b < blocks:
            a_copy(b).wait()
        if b >= 1:
            g_first(b - 1).wait()
        if b < blocks:
            a_t[:, b * rows_a:(b + 1) * rows_a] = a_raw[b % RAW].T
        if b >= 1:
            k = slice((b - 1) * rows_a, b * rows_a)
            new = jnp.dot(a_t[:, k], g_buf[0, k, :], preferred_element_type=f32)
            part[...] = new if b == 1 else part[...] + new
        if b + RAW < blocks:
            g_first(b + RAW).start()
        if b < blocks:
            a_copy(b + RAW).start()
        if b == blocks - 1:
            g_copy(1).start()
    d2d_out[...] = part[pl.ds(theirs, half), :].astype(bf16)
    pl.semaphore_wait(barrier, 3)
    d2d(0).start()
    pair(0)

    @pl.loop(1, steps)
    def _(s):
        @pl.when(s % per == 0)
        def _():
            @pl.loop(s // per * blocks, s // per * blocks + blocks)
            def _(b):
                a_copy(b).wait()
                a_t[:, pl.ds(pl.multiple_of((b % blocks) * rows_a, rows_a), rows_a)] = a_raw[b % RAW].T
                pl.when(b + RAW < mats * blocks)(lambda: a_copy(b + RAW).start())

        g_copy(s).wait()
        pl.when(s + 1 < steps)(lambda: g_copy(s + 1).start())
        d2d_out[...] = dot(theirs, s).astype(bf16)
        d2d(s).start()
        events(s, 0)
        part[pl.ds(mine, half), :] = dot(mine, s)
        pair(s)
        events(s, 1)

    @pl.loop(steps, steps + AG3 + 1)
    def _(s):
        events(s, 0)
        events(s, 1)


def spread(held, o_ref, sem):
    mats, d, _ = o_ref.shape
    pieces = sem.shape[0] // mats
    rows = d // pieces
    copies = []
    for i in range(mats * pieces):
        at = (i // pieces, pl.ds(i % pieces * rows, rows))
        copies.append(pltpu.make_async_copy(held.at[at], o_ref.at[at], sem.at[i]))
    for c in copies:
        c.start()
    for c in copies:
        c.wait()


def solution(mesh):
    def step(a, g):
        _, mats, tokens, d = a.shape
        ff = g.shape[-1]
        width = 512 if ff % 512 == 0 else ff
        blocks = ff // width
        half, quarter, eighth = d // 2, d // 4, d // 8
        f32, bf16 = jnp.float32, jnp.bfloat16
        dma = pltpu.SemaphoreType.DMA
        held = pl.pallas_call(
            functools.partial(kernel, (mats, tokens, d, ff, width, blocks)),
            out_shape=pltpu.VMEM((mats, d, ff), bf16),
            in_specs=[pl.BlockSpec(memory_space=pl.ANY)] * 2,
            out_specs=pl.BlockSpec(memory_space=pltpu.VMEM),
            scratch_shapes=[
                pltpu.VMEM((RAW, tokens // blocks, d), bf16),
                pltpu.VMEM((d, tokens), bf16),
                pltpu.VMEM((2, tokens, width), bf16),
                pltpu.VMEM((half, width), bf16),
                pltpu.VMEM((2, half, width), bf16),
                pltpu.VMEM((d, width), f32),
                pltpu.VMEM((SLOTS, quarter, width), f32),
                pltpu.VMEM((SLOTS, quarter, width), bf16),
                pltpu.VMEM((SLOTS, quarter, width), bf16),
                pltpu.VMEM((SLOTS, eighth, width), f32),
                pltpu.VMEM((SLOTS, eighth, width), bf16),
                pltpu.VMEM((SLOTS, eighth, width), bf16),
                dma((RAW,)), dma((2,)), dma((blocks,)), dma((1,)), dma((2,)),
                *[dma((2 * SLOTS,)) for _ in range(4)], *[dma((2 * HELD,)) for _ in range(6)],
            ],
            compiler_params=pltpu.CompilerParams(
                collective_id=0, has_side_effects=True, vmem_limit_bytes=31 * 2**20 + 2**19
            ),
        )(a, g)
        return pl.pallas_call(
            spread,
            out_shape=jax.ShapeDtypeStruct((mats, d, ff), bf16),
            in_specs=[pl.BlockSpec(memory_space=pltpu.VMEM)],
            out_specs=pl.BlockSpec(memory_space=pl.ANY),
            scratch_shapes=[dma((4 * mats,))],
            compiler_params=pltpu.CompilerParams(vmem_limit_bytes=2**20),
        )(held)

    spec = P(("rep", "dp"), None, None, None)
    return jax.shard_map(step, mesh=mesh, in_specs=(spec, spec), out_specs=P("rep", None, None), check_vma=False)
```

```python
import functools

import jax
import jax.numpy as jnp
from jax import lax
from jax.experimental import pallas as pl
from jax.experimental.pallas import tpu as pltpu
from jax.sharding import PartitionSpec as P

MESH = pl.DeviceIdType.MESH
SLOTS = 4
HELD = 8
TAIL = 4
RAW = 4
RS1, RS2, AG1, AG2, AG3 = 1, 2, 3, 5, 6


def flip(i, bit):
    return i + bit - 2 * bit * ((i // bit) % 2)


def kernel(
    cfg, a_ref, g_ref, o_ref, tail_ref,
    a_raw, a_t, g_buf, d2d_out, d2d_in, part, keep1, rs1_out, rs1_in, keep2, rs2_out, rs2_in,
    a_sem, g_sem, g0_sem, d2d_s, d2d_r, rs1_s, rs1_r, rs2_s, rs2_r, ag1_s, ag1_r, ag2_s, ag2_r, ag3_s, ag3_r,
):
    mats, tokens, d, ff, width, blocks = cfg
    per = ff // width
    steps = mats * per
    half, quarter, eighth = d // 2, d // 4, d // 8
    rows_a = tokens // blocks
    f32, bf16 = jnp.float32, jnp.bfloat16

    me = lax.axis_index("dp")
    core, y, x = me % 2, (me // 2) % 2, (me // 4) % 2
    cu = x + core * (y - x)
    cv = y + core * (x - y)
    mate = flip(me, 1)
    at_x, at_y = flip(me, 4), flip(me, 2)
    u = at_x + core * (at_y - at_x)
    v = at_y + core * (at_x - at_y)

    mine = pl.multiple_of(core * half, half)
    theirs = pl.multiple_of((1 - core) * half, half)
    e_keep = pl.ds(pl.multiple_of(cv * eighth, eighth), eighth)
    e_send = pl.ds(pl.multiple_of((1 - cv) * eighth, eighth), eighth)
    rows_h = pl.ds(mine, half)
    order = (
        theirs + (1 - cv) * quarter, mine + (1 - cu) * quarter, theirs + cv * quarter, mine + cu * quarter
    )
    send_theirs, send_mine, keep_theirs, keep_mine = (pl.ds(i * quarter, quarter) for i in range(4))
    rows_q = pl.ds(pl.multiple_of(mine + cu * quarter, quarter), quarter)
    e_keep = pl.ds(pl.multiple_of(cv * eighth, eighth), eighth)
    e_send = pl.ds(pl.multiple_of((1 - cv) * eighth, eighth), eighth)
    rows_h = pl.ds(mine, half)
    rows_send = pl.ds(pl.multiple_of(mine + (1 - cu) * quarter, quarter), quarter)
    rows_mate = [pl.ds(pl.multiple_of(theirs + c * quarter, quarter), quarter) for c in (1 - cv, cv)]
    rows_q = pl.ds(pl.multiple_of(mine + cu * quarter, quarter), quarter)
    rows_e = pl.ds(pl.multiple_of(mine + cu * quarter + cv * eighth, eighth), eighth)

    def remote(src, dst, s_sem, r_sem, to):
        return pltpu.make_async_remote_copy(
            src_ref=src, dst_ref=dst, send_sem=s_sem, recv_sem=r_sem, device_id={"dp": to}, device_id_type=MESH
        )

    part_w = width // 2

    def cols(k):
        return pl.ds(pl.multiple_of((k % per) * width, width), width)

    def cols_of(k, p):
        return pl.ds(pl.multiple_of((k % per) * width + p * part_w, part_w), part_w)

    def lanes(p):
        return pl.ds(p * part_w, part_w)

    def g_copy(s):
        return pltpu.make_async_copy(g_ref.at[0, s // per, :, cols(s)], g_buf.at[s % 2], g_sem.at[s % 2])

    def g_first(b):
        rows = pl.ds(b * rows_a, rows_a)
        return pltpu.make_async_copy(g_ref.at[0, 0, rows, pl.ds(0, width)], g_buf.at[0, rows, :], g0_sem.at[b])

    class a_copy:
        def __init__(self, b, f):
            i = b % RAW
            rows = pl.ds(pl.multiple_of((b % blocks) * rows_a, rows_a), rows_a)
            self.copies = [
                pltpu.make_async_copy(
                    a_ref.at[0, b // blocks, rows, pl.ds(pl.multiple_of(order[2 * f + c], quarter), quarter)],
                    a_raw.at[f, i, :, pl.ds(c * quarter, quarter)],
                    a_sem.at[(2 * f + c) * RAW + i],
                )
                for c in range(2)
            ]

        def start(self):
            for c in self.copies:
                c.start()

        def wait(self):
            for c in self.copies:
                c.wait()

    def d2d(s, q):
        i = s % 2
        return remote(d2d_out.at[q], d2d_in.at[i, q], d2d_s.at[q], d2d_r.at[i * 2 + q], mate)

    def rs1(k, p):
        i, j = k % SLOTS, k % SLOTS * 2 + p
        return remote(rs1_out.at[i, :, lanes(p)], rs1_in.at[i, :, lanes(p)], rs1_s.at[j], rs1_r.at[j], u)

    def rs2(k, p):
        i, j = k % SLOTS, k % SLOTS * 2 + p
        return remote(rs2_out.at[i, :, lanes(p)], rs2_in.at[i, :, lanes(p)], rs2_s.at[j], rs2_r.at[j], v)

    def gather(k, p, rows, s_sem, r_sem, to):
        j = k % HELD * 2 + p
        r = o_ref.at[k // per, rows, cols_of(k, p)]
        return remote(r, r, s_sem.at[j], r_sem.at[j], to)

    def ag1(k, p):
        return gather(k, p, rows_e, ag1_s, ag1_r, v)

    def ag2(k, p):
        return gather(k, p, rows_q, ag2_s, ag2_r, u)

    def ag3(k, p):
        return gather(k, p, rows_h, ag3_s, ag3_r, mate)

    def at(s, lag, end=steps):
        def run(f):
            k = s - lag
            pl.when(jnp.logical_and(k >= 0, k < end))(lambda: f(k))
        return run

    def events(s, p):
        c = lanes(p)

        @at(s, AG3, steps - (TAIL + p) // 2)
        def _(k):
            ag3(k, p).wait()

        @at(s, AG2, steps - (TAIL + p) // 2)
        def _(k):
            ag2(k, p).wait()
            ag3(k, p).start()

        @at(s, AG1)
        def _(k):
            ag1(k, p).wait()
            tail = 2 * (k - steps) + p + TAIL
            pl.when(tail < 0)(lambda: ag2(k, p).start())

            @pl.when(tail >= 0)
            def _():
                to = pl.ds(pl.multiple_of(tail * part_w, part_w), part_w)
                tail_ref[:, to] = o_ref[mats - 1, rows_q, cols_of(k, p)]

        @at(s, RS2)
        def _(k):
            rs2(k, p).wait()
            i = k % SLOTS
            o_ref[k // per, rows_e, cols_of(k, p)] = (keep2[i, :, c] + rs2_in[i, :, c].astype(f32)).astype(bf16)
            ag1(k, p).start()

        @at(s, RS1)
        def _(k):
            rs1(k, p).wait()
            i = k % SLOTS
            rs2_out[i, :, c] = (keep1[i, e_send, c] + rs1_in[i, e_send, c].astype(f32)).astype(bf16)
            rs2(k, p).start()
            keep2[i, :, c] = keep1[i, e_keep, c] + rs1_in[i, e_keep, c].astype(f32)

    def send_on(s, product):
        d2d(s, 0).wait()
        i, h = s % SLOTS, s % 2
        rs1_out[i] = (product() + d2d_in[h, 0].astype(f32)).astype(bf16)
        for p in range(2):
            rs1(s, p).start()

    def keep(s, product):
        d2d(s, 1).wait()
        i, h = s % SLOTS, s % 2
        keep1[i] = product() + d2d_in[h, 1].astype(f32)

    for b in range(RAW):
        a_copy(b, 0).start()
        g_first(b).start()

    barrier = pltpu.get_barrier_semaphore()
    for peer in (mate, u, v):
        pl.semaphore_signal(barrier, inc=1, device_id={"dp": peer}, device_id_type=MESH)

    for f in range(2):
        to = slice(2 * f * quarter, 2 * (f + 1) * quarter)
        for b in range(blocks + 1):
            if b < blocks:
                a_copy(b, f).wait()
            if b >= 1 and f == 0:
                g_first(b - 1).wait()
            if b < blocks:
                a_t[to, b * rows_a:(b + 1) * rows_a] = a_raw[f, b % RAW].T
            if b >= 1:
                k = slice((b - 1) * rows_a, b * rows_a)
                new = jnp.dot(a_t[to, k], g_buf[0, k, :], preferred_element_type=f32)
                part[to, :] = new if b == 1 else part[to, :] + new
            if b + RAW < blocks:
                a_copy(b + RAW, f).start()
                if f == 0:
                    g_first(b + RAW).start()
            elif b < blocks:
                if f == 0:
                    a_copy(b + RAW - blocks, 1).start()
                else:
                    a_copy(b + RAW, 0).start()
                    a_copy(b + RAW, 1).start()
            if f == 1 and b == blocks // 2:
                g_copy(1).start()
                send_on(0, lambda: part[send_mine, :])
        if f == 0:
            pl.semaphore_wait(barrier, 3)
        d2d_out[f] = part[(send_theirs, keep_theirs)[f], :].astype(bf16)
        d2d(0, f).start()

    @pl.loop(1, steps)
    def _(s):
        @pl.when(s % per == 0)
        def _():
            @pl.loop(s // per * blocks, s // per * blocks + blocks)
            def _(b):
                for f in range(2):
                    a_copy(b, f).wait()
                    blk = pl.ds(pl.multiple_of((b % blocks) * rows_a, rows_a), rows_a)
                    a_t[2 * f * quarter:2 * (f + 1) * quarter, blk] = a_raw[f, b % RAW].T
                    pl.when(b + RAW < mats * blocks)(lambda: a_copy(b + RAW, f).start())

        g_copy(s).wait()
        pl.when(s + 1 < steps)(lambda: g_copy(s + 1).start())
        def product(rows):
            return jnp.dot(a_t[rows, :], g_buf[s % 2], preferred_element_type=f32)

        d2d_out[0] = product(send_theirs).astype(bf16)
        d2d(s, 0).start()
        pl.when(s == 1)(lambda: keep(0, lambda: part[keep_mine, :]))
        d2d_out[1] = product(keep_theirs).astype(bf16)
        d2d(s, 1).start()
        events(s, 0)
        send_on(s, lambda: product(send_mine))
        keep(s, lambda: product(keep_mine))
        events(s, 1)

    @pl.loop(steps, steps + AG3 + 1)
    def _(s):
        events(s, 0)
        events(s, 1)


def place(me, d):
    half, quarter = d // 2, d // 4
    core, y, x = me % 2, (me // 2) % 2, (me // 4) % 2
    cu, cv = x + core * (y - x), y + core * (x - y)
    starts = (
        core * half + cu * quarter, core * half + (1 - cu) * quarter,
        (1 - core) * half + cv * quarter, (1 - core) * half + (1 - cv) * quarter,
    )
    return [pl.ds(pl.multiple_of(i, quarter), quarter) for i in starts]


def spread(tail, held, o_ref, sem):
    mats, d, ff = o_ref.shape
    own = place(lax.axis_index("dp"), d)[0]
    parts = [(n, pl.ds(i * (d // 4), d // 4), pl.ds(0, ff)) for n in range(mats - 1) for i in range(4)]
    parts += [(mats - 1, pl.ds(i * (d // 4), d // 4), pl.ds(0, ff - tail)) for i in range(4)]
    parts += [(mats - 1, own, pl.ds(ff - tail, tail))]
    copies = [pltpu.make_async_copy(held.at[p], o_ref.at[p], sem.at[i]) for i, p in enumerate(parts)]
    for c in copies:
        c.start()
    for c in copies:
        c.wait()


def finish(from_u, from_mate, from_far, _, o_ref, sem):
    mats, d, ff = o_ref.shape
    tail = from_u.shape[1]
    rows = place(lax.axis_index("dp"), d)[1:]
    copies = [
        pltpu.make_async_copy(piece, o_ref.at[mats - 1, r, pl.ds(ff - tail, tail)], sem.at[i])
        for i, (piece, r) in enumerate(zip((from_u, from_mate, from_far), rows))
    ]
    for c in copies:
        c.start()
    for c in copies:
        c.wait()


def solution(mesh):
    def step(a, g):
        _, mats, tokens, d = a.shape
        ff = g.shape[-1]
        width = 512 if ff % 512 == 0 else ff
        blocks = ff // width
        half, quarter, eighth = d // 2, d // 4, d // 8
        f32, bf16 = jnp.float32, jnp.bfloat16
        dma = pltpu.SemaphoreType.DMA
        tail = TAIL * width // 2
        held, quarters = pl.pallas_call(
            functools.partial(kernel, (mats, tokens, d, ff, width, blocks)),
            out_shape=(pltpu.VMEM((mats, d, ff), bf16), pltpu.VMEM((quarter, tail), bf16)),
            in_specs=[pl.BlockSpec(memory_space=pl.ANY)] * 2,
            out_specs=(pl.BlockSpec(memory_space=pltpu.VMEM), pl.BlockSpec(memory_space=pltpu.VMEM)),
            scratch_shapes=[
                pltpu.VMEM((2, RAW, tokens // blocks, half), bf16),
                pltpu.VMEM((d, tokens), bf16),
                pltpu.VMEM((2, tokens, width), bf16),
                pltpu.VMEM((2, quarter, width), bf16),
                pltpu.VMEM((2, 2, quarter, width), bf16),
                pltpu.VMEM((d, width), f32),
                pltpu.VMEM((SLOTS, quarter, width), f32),
                pltpu.VMEM((SLOTS, quarter, width), bf16),
                pltpu.VMEM((SLOTS, quarter, width), bf16),
                pltpu.VMEM((SLOTS, eighth, width), f32),
                pltpu.VMEM((SLOTS, eighth, width), bf16),
                pltpu.VMEM((SLOTS, eighth, width), bf16),
                dma((4 * RAW,)), dma((2,)), dma((blocks,)), dma((2,)), dma((4,)),
                *[dma((2 * SLOTS,)) for _ in range(4)], *[dma((2 * HELD,)) for _ in range(6)],
            ],
            compiler_params=pltpu.CompilerParams(
                collective_id=0, has_side_effects=True, vmem_limit_bytes=31 * 2**20
            ),
        )(a, g)
        devices = range(mesh.shape["dp"])
        near = [flip(i, 2 if i % 2 else 4) for i in devices]
        send = lambda to: lax.ppermute(quarters, "dp", [(i, to[i]) for i in devices])
        from_u = send(near)
        from_far = send([flip(i, 1) for i in near])
        from_mate = send([flip(i, 1) for i in devices])
        whole = jax.ShapeDtypeStruct((mats, d, ff), bf16)
        out = pl.pallas_call(
            functools.partial(spread, tail),
            out_shape=whole,
            in_specs=[pl.BlockSpec(memory_space=pltpu.VMEM)],
            out_specs=pl.BlockSpec(memory_space=pl.ANY),
            scratch_shapes=[dma((4 * mats + 1,))],
            compiler_params=pltpu.CompilerParams(vmem_limit_bytes=2**20),
            cost_estimate=pl.CostEstimate(flops=10**10, bytes_accessed=2 * mats * d * ff * 2, transcendentals=0),
        )(held)
        return pl.pallas_call(
            finish,
            out_shape=whole,
            in_specs=[pl.BlockSpec(memory_space=pltpu.VMEM)] * 3 + [pl.BlockSpec(memory_space=pl.ANY)],
            out_specs=pl.BlockSpec(memory_space=pl.ANY),
            scratch_shapes=[dma((3,))],
            input_output_aliases={3: 0},
            compiler_params=pltpu.CompilerParams(vmem_limit_bytes=8 * 2**20),
        )(from_u, from_mate, from_far, out)

    spec = P(("rep", "dp"), None, None, None)
    return jax.shard_map(step, mesh=mesh, in_specs=(spec, spec), out_specs=P("rep", None, None), check_vma=False)
```

```python
import functools

import jax
import jax.numpy as jnp
from jax import lax
from jax.experimental import pallas as pl
from jax.experimental.pallas import tpu as pltpu
from jax.sharding import PartitionSpec as P

MESH = pl.DeviceIdType.MESH
SLOTS = 4
HELD = 8
TAIL = 5
RAW = 4
RS1, RS2, AG1, AG2, AG3 = 1, 2, 3, 5, 6


def flip(i, bit):
    return i + bit - 2 * bit * ((i // bit) % 2)


def kernel(
    cfg, a_ref, g_ref, o_ref, tail_ref,
    a_raw, a_t, g_buf, d2d_out, d2d_in, part, keep1, rs1_out, rs1_in, keep2, rs2_out, rs2_in,
    a_sem, g_sem, g0_sem, d2d_s, d2d_r, rs1_s, rs1_r, rs2_s, rs2_r, ag1_s, ag1_r, ag2_s, ag2_r, ag3_s, ag3_r,
):
    mats, tokens, d, ff, width, blocks = cfg
    per = ff // width
    steps = mats * per
    half, quarter, eighth = d // 2, d // 4, d // 8
    rows_a = tokens // blocks
    f32, bf16 = jnp.float32, jnp.bfloat16

    me = lax.axis_index("dp")
    core, y, x = me % 2, (me // 2) % 2, (me // 4) % 2
    cu = x + core * (y - x)
    cv = y + core * (x - y)
    mate = flip(me, 1)
    at_x, at_y = flip(me, 4), flip(me, 2)
    u = at_x + core * (at_y - at_x)
    v = at_y + core * (at_x - at_y)

    mine = pl.multiple_of(core * half, half)
    theirs = pl.multiple_of((1 - core) * half, half)
    e_keep = pl.ds(pl.multiple_of(cv * eighth, eighth), eighth)
    e_send = pl.ds(pl.multiple_of((1 - cv) * eighth, eighth), eighth)
    rows_h = pl.ds(mine, half)
    order = (
        theirs + (1 - cv) * quarter, mine + (1 - cu) * quarter, theirs + cv * quarter, mine + cu * quarter
    )
    send_theirs, send_mine, keep_theirs, keep_mine = (pl.ds(i * quarter, quarter) for i in range(4))
    rows_q = pl.ds(pl.multiple_of(mine + cu * quarter, quarter), quarter)
    e_keep = pl.ds(pl.multiple_of(cv * eighth, eighth), eighth)
    e_send = pl.ds(pl.multiple_of((1 - cv) * eighth, eighth), eighth)
    rows_h = pl.ds(mine, half)
    rows_send = pl.ds(pl.multiple_of(mine + (1 - cu) * quarter, quarter), quarter)
    rows_mate = [pl.ds(pl.multiple_of(theirs + c * quarter, quarter), quarter) for c in (1 - cv, cv)]
    rows_q = pl.ds(pl.multiple_of(mine + cu * quarter, quarter), quarter)
    rows_e = pl.ds(pl.multiple_of(mine + cu * quarter + cv * eighth, eighth), eighth)

    def remote(src, dst, s_sem, r_sem, to):
        return pltpu.make_async_remote_copy(
            src_ref=src, dst_ref=dst, send_sem=s_sem, recv_sem=r_sem, device_id={"dp": to}, device_id_type=MESH
        )

    part_w = width // 2

    def cols(k):
        return pl.ds(pl.multiple_of((k % per) * width, width), width)

    def cols_of(k, p):
        return pl.ds(pl.multiple_of((k % per) * width + p * part_w, part_w), part_w)

    def lanes(p):
        return pl.ds(p * part_w, part_w)

    def g_copy(s):
        return pltpu.make_async_copy(g_ref.at[0, s // per, :, cols(s)], g_buf.at[s % 2], g_sem.at[s % 2])

    def g_first(b):
        rows = pl.ds(b * rows_a, rows_a)
        return pltpu.make_async_copy(g_ref.at[0, 0, rows, pl.ds(0, width)], g_buf.at[0, rows, :], g0_sem.at[b])

    class a_copy:
        def __init__(self, b, f):
            i = b % RAW
            rows = pl.ds(pl.multiple_of((b % blocks) * rows_a, rows_a), rows_a)
            self.copies = [
                pltpu.make_async_copy(
                    a_ref.at[0, b // blocks, rows, pl.ds(pl.multiple_of(order[2 * f + c], quarter), quarter)],
                    a_raw.at[f, i, :, pl.ds(c * quarter, quarter)],
                    a_sem.at[(2 * f + c) * RAW + i],
                )
                for c in range(2)
            ]

        def start(self):
            for c in self.copies:
                c.start()

        def wait(self):
            for c in self.copies:
                c.wait()

    def d2d(s, q):
        i = s % 2
        return remote(d2d_out.at[q], d2d_in.at[i, q], d2d_s.at[q], d2d_r.at[i * 2 + q], mate)

    def rs1(k, p):
        i, j = k % SLOTS, k % SLOTS * 2 + p
        return remote(rs1_out.at[i, :, lanes(p)], rs1_in.at[i, :, lanes(p)], rs1_s.at[j], rs1_r.at[j], u)

    def rs2(k, p):
        i, j = k % SLOTS, k % SLOTS * 2 + p
        return remote(rs2_out.at[i, :, lanes(p)], rs2_in.at[i, :, lanes(p)], rs2_s.at[j], rs2_r.at[j], v)

    def gather(k, p, rows, s_sem, r_sem, to):
        j = k % HELD * 2 + p
        r = o_ref.at[k // per, rows, cols_of(k, p)]
        return remote(r, r, s_sem.at[j], r_sem.at[j], to)

    def ag1(k, p):
        return gather(k, p, rows_e, ag1_s, ag1_r, v)

    def ag2(k, p):
        return gather(k, p, rows_q, ag2_s, ag2_r, u)

    def ag3(k, p):
        return gather(k, p, rows_h, ag3_s, ag3_r, mate)

    def at(s, lag, end=steps):
        def run(f):
            k = s - lag
            pl.when(jnp.logical_and(k >= 0, k < end))(lambda: f(k))
        return run

    def events(s, p):
        c = lanes(p)

        @at(s, AG3, steps - (TAIL + p) // 2)
        def _(k):
            ag3(k, p).wait()

        @at(s, AG2, steps - (TAIL + p) // 2)
        def _(k):
            ag2(k, p).wait()
            ag3(k, p).start()

        @at(s, AG1)
        def _(k):
            ag1(k, p).wait()
            tail = 2 * (k - steps) + p + TAIL
            pl.when(tail < 0)(lambda: ag2(k, p).start())

            @pl.when(tail >= 0)
            def _():
                to = pl.ds(pl.multiple_of(tail * part_w, part_w), part_w)
                tail_ref[:, to] = o_ref[mats - 1, rows_q, cols_of(k, p)]

        @at(s, RS2)
        def _(k):
            rs2(k, p).wait()
            i = k % SLOTS
            o_ref[k // per, rows_e, cols_of(k, p)] = (keep2[i, :, c] + rs2_in[i, :, c].astype(f32)).astype(bf16)
            ag1(k, p).start()

        @at(s, RS1)
        def _(k):
            rs1(k, p).wait()
            i = k % SLOTS
            rs2_out[i, :, c] = (keep1[i, e_send, c] + rs1_in[i, e_send, c].astype(f32)).astype(bf16)
            rs2(k, p).start()
            keep2[i, :, c] = keep1[i, e_keep, c] + rs1_in[i, e_keep, c].astype(f32)

    def send_on(s, product):
        d2d(s, 0).wait()
        i, h = s % SLOTS, s % 2
        rs1_out[i] = (product() + d2d_in[h, 0].astype(f32)).astype(bf16)
        for p in range(2):
            rs1(s, p).start()

    def keep(s, product):
        d2d(s, 1).wait()
        i, h = s % SLOTS, s % 2
        keep1[i] = product() + d2d_in[h, 1].astype(f32)

    for b in range(RAW):
        a_copy(b, 0).start()
        g_first(b).start()

    barrier = pltpu.get_barrier_semaphore()
    for peer in (mate, u, v):
        pl.semaphore_signal(barrier, inc=1, device_id={"dp": peer}, device_id_type=MESH)

    for f in range(2):
        to = slice(2 * f * quarter, 2 * (f + 1) * quarter)
        for b in range(blocks + 1):
            if b < blocks:
                a_copy(b, f).wait()
            if b >= 1 and f == 0:
                g_first(b - 1).wait()
            if b < blocks:
                a_t[to, b * rows_a:(b + 1) * rows_a] = a_raw[f, b % RAW].T
            if b >= 1:
                k = slice((b - 1) * rows_a, b * rows_a)
                new = jnp.dot(a_t[to, k], g_buf[0, k, :], preferred_element_type=f32)
                part[to, :] = new if b == 1 else part[to, :] + new
            if b + RAW < blocks:
                a_copy(b + RAW, f).start()
                if f == 0:
                    g_first(b + RAW).start()
            elif b < blocks:
                if f == 0:
                    a_copy(b + RAW - blocks, 1).start()
                else:
                    a_copy(b + RAW, 0).start()
                    a_copy(b + RAW, 1).start()
            if f == 1 and b == blocks // 2:
                g_copy(1).start()
                send_on(0, lambda: part[send_mine, :])
        if f == 0:
            pl.semaphore_wait(barrier, 3)
        d2d_out[f] = part[(send_theirs, keep_theirs)[f], :].astype(bf16)
        d2d(0, f).start()

    @pl.loop(1, steps)
    def _(s):
        @pl.when(s % per == 0)
        def _():
            @pl.loop(s // per * blocks, s // per * blocks + blocks)
            def _(b):
                for f in range(2):
                    a_copy(b, f).wait()
                    blk = pl.ds(pl.multiple_of((b % blocks) * rows_a, rows_a), rows_a)
                    a_t[2 * f * quarter:2 * (f + 1) * quarter, blk] = a_raw[f, b % RAW].T
                    pl.when(b + RAW < mats * blocks)(lambda: a_copy(b + RAW, f).start())

        g_copy(s).wait()
        pl.when(s + 1 < steps)(lambda: g_copy(s + 1).start())
        def product(rows):
            return jnp.dot(a_t[rows, :], g_buf[s % 2], preferred_element_type=f32)

        d2d_out[0] = product(send_theirs).astype(bf16)
        d2d(s, 0).start()
        pl.when(s == 1)(lambda: keep(0, lambda: part[keep_mine, :]))
        d2d_out[1] = product(keep_theirs).astype(bf16)
        d2d(s, 1).start()
        events(s, 0)
        send_on(s, lambda: product(send_mine))
        keep(s, lambda: product(keep_mine))
        events(s, 1)

    @pl.loop(steps, steps + AG3 + 1)
    def _(s):
        events(s, 0)
        events(s, 1)


def place(me, d):
    half, quarter = d // 2, d // 4
    core, y, x = me % 2, (me // 2) % 2, (me // 4) % 2
    cu, cv = x + core * (y - x), y + core * (x - y)
    starts = (
        core * half + cu * quarter, core * half + (1 - cu) * quarter,
        (1 - core) * half + cv * quarter, (1 - core) * half + (1 - cv) * quarter,
    )
    return [pl.ds(pl.multiple_of(i, quarter), quarter) for i in starts]


def run(copies):
    for c in copies:
        c.start()
    for c in copies:
        c.wait()


def spread(held, o_ref, sem):
    mats, d, ff = o_ref.shape
    parts = [(n, pl.ds(i * (d // 4), d // 4)) for n in range(mats - 1) for i in range(4)]
    run([pltpu.make_async_copy(held.at[p], o_ref.at[p], sem.at[i]) for i, p in enumerate(parts)])


def spread_last(tail, held, _, o_ref, sem):
    mats, d, ff = o_ref.shape
    own = place(lax.axis_index("dp"), d)[0]
    parts = [(mats - 1, pl.ds(i * (d // 4), d // 4), pl.ds(0, ff - tail)) for i in range(4)]
    parts += [(mats - 1, own, pl.ds(ff - tail, tail))]
    run([pltpu.make_async_copy(held.at[p], o_ref.at[p], sem.at[i]) for i, p in enumerate(parts)])


def finish(from_u, from_mate, from_far, _, o_ref, sem):
    mats, d, ff = o_ref.shape
    tail = from_u.shape[1]
    rows = place(lax.axis_index("dp"), d)[1:]
    run([
        pltpu.make_async_copy(piece, o_ref.at[mats - 1, r, pl.ds(ff - tail, tail)], sem.at[i])
        for i, (piece, r) in enumerate(zip((from_u, from_mate, from_far), rows))
    ])


def solution(mesh):
    def step(a, g):
        _, mats, tokens, d = a.shape
        ff = g.shape[-1]
        width = 512 if ff % 512 == 0 else ff
        blocks = ff // width
        half, quarter, eighth = d // 2, d // 4, d // 8
        f32, bf16 = jnp.float32, jnp.bfloat16
        dma = pltpu.SemaphoreType.DMA
        tail = TAIL * width // 2
        held, quarters = pl.pallas_call(
            functools.partial(kernel, (mats, tokens, d, ff, width, blocks)),
            out_shape=(pltpu.VMEM((mats, d, ff), bf16), pltpu.VMEM((quarter, tail), bf16)),
            in_specs=[pl.BlockSpec(memory_space=pl.ANY)] * 2,
            out_specs=(pl.BlockSpec(memory_space=pltpu.VMEM), pl.BlockSpec(memory_space=pltpu.VMEM)),
            scratch_shapes=[
                pltpu.VMEM((2, RAW, tokens // blocks, half), bf16),
                pltpu.VMEM((d, tokens), bf16),
                pltpu.VMEM((2, tokens, width), bf16),
                pltpu.VMEM((2, quarter, width), bf16),
                pltpu.VMEM((2, 2, quarter, width), bf16),
                pltpu.VMEM((d, width), f32),
                pltpu.VMEM((SLOTS, quarter, width), f32),
                pltpu.VMEM((SLOTS, quarter, width), bf16),
                pltpu.VMEM((SLOTS, quarter, width), bf16),
                pltpu.VMEM((SLOTS, eighth, width), f32),
                pltpu.VMEM((SLOTS, eighth, width), bf16),
                pltpu.VMEM((SLOTS, eighth, width), bf16),
                dma((4 * RAW,)), dma((2,)), dma((blocks,)), dma((2,)), dma((4,)),
                *[dma((2 * SLOTS,)) for _ in range(4)], *[dma((2 * HELD,)) for _ in range(6)],
            ],
            compiler_params=pltpu.CompilerParams(
                collective_id=0, has_side_effects=True, vmem_limit_bytes=31 * 2**20
            ),
        )(a, g)
        devices = range(mesh.shape["dp"])
        send = lambda x, to: lax.ppermute(x, "dp", [(i, to[i]) for i in devices])
        mates = [flip(i, 1) for i in devices]
        from_u = send(quarters, [flip(i, 2 if i % 2 else 4) for i in devices])
        from_mate = send(quarters, mates)
        from_far = send(from_u, mates)
        whole = jax.ShapeDtypeStruct((mats, d, ff), bf16)
        cost = lambda n: pl.CostEstimate(flops=n * 10**10, bytes_accessed=2 * n * d * ff * 2, transcendentals=0)
        out = pl.pallas_call(
            spread,
            out_shape=whole,
            in_specs=[pl.BlockSpec(memory_space=pltpu.VMEM)],
            out_specs=pl.BlockSpec(memory_space=pl.ANY),
            scratch_shapes=[dma((4 * mats,))],
            compiler_params=pltpu.CompilerParams(vmem_limit_bytes=2**20),
            cost_estimate=cost(mats - 1),
        )(held)
        out = pl.pallas_call(
            functools.partial(spread_last, tail),
            out_shape=whole,
            in_specs=[pl.BlockSpec(memory_space=pltpu.VMEM), pl.BlockSpec(memory_space=pl.ANY)],
            out_specs=pl.BlockSpec(memory_space=pl.ANY),
            scratch_shapes=[dma((5,))],
            input_output_aliases={1: 0},
            compiler_params=pltpu.CompilerParams(vmem_limit_bytes=2**20),
            cost_estimate=cost(1),
        )(held, out)
        return pl.pallas_call(
            finish,
            out_shape=whole,
            in_specs=[pl.BlockSpec(memory_space=pltpu.VMEM)] * 3 + [pl.BlockSpec(memory_space=pl.ANY)],
            out_specs=pl.BlockSpec(memory_space=pl.ANY),
            scratch_shapes=[dma((3,))],
            input_output_aliases={3: 0},
            compiler_params=pltpu.CompilerParams(vmem_limit_bytes=8 * 2**20),
        )(from_u, from_mate, from_far, out)

    spec = P(("rep", "dp"), None, None, None)
    return jax.shard_map(step, mesh=mesh, in_specs=(spec, spec), out_specs=P("rep", None, None), check_vma=False)
```

```python
import functools

import jax
import jax.numpy as jnp
from jax import lax
from jax.experimental import pallas as pl
from jax.experimental.pallas import tpu as pltpu
from jax.sharding import PartitionSpec as P

EARLY = 5
MESH = pl.DeviceIdType.MESH
SLOTS = 4
HELD = 8
TAIL = 5
RAW = 4
RS1, RS2, AG1, AG2, AG3 = 1, 2, 3, 5, 6


def flip(i, bit):
    return i + bit - 2 * bit * ((i // bit) % 2)


def kernel(
    cfg, a_ref, g_ref, o_ref, tail_ref,
    a_raw, a_t, g_buf, d2d_out, d2d_in, part, keep1, rs1_out, rs1_in, keep2, rs2_out, rs2_in,
    a_sem, g_sem, g0_sem, d2d_s, d2d_r, rs1_s, rs1_r, rs2_s, rs2_r, ag1_s, ag1_r, ag2_s, ag2_r, ag3_s, ag3_r,
):
    mats, tokens, d, ff, width, blocks = cfg
    per = ff // width
    steps = mats * per
    half, quarter, eighth = d // 2, d // 4, d // 8
    rows_a = tokens // blocks
    f32, bf16 = jnp.float32, jnp.bfloat16

    me = lax.axis_index("dp")
    core, y, x = me % 2, (me // 2) % 2, (me // 4) % 2
    cu = x + core * (y - x)
    cv = y + core * (x - y)
    mate = flip(me, 1)
    at_x, at_y = flip(me, 4), flip(me, 2)
    u = at_x + core * (at_y - at_x)
    v = at_y + core * (at_x - at_y)

    mine = pl.multiple_of(core * half, half)
    theirs = pl.multiple_of((1 - core) * half, half)
    e_keep = pl.ds(pl.multiple_of(cv * eighth, eighth), eighth)
    e_send = pl.ds(pl.multiple_of((1 - cv) * eighth, eighth), eighth)
    rows_h = pl.ds(mine, half)
    order = (
        theirs + (1 - cv) * quarter, mine + (1 - cu) * quarter, theirs + cv * quarter, mine + cu * quarter
    )
    send_theirs, send_mine, keep_theirs, keep_mine = (pl.ds(i * quarter, quarter) for i in range(4))
    rows_q = pl.ds(pl.multiple_of(mine + cu * quarter, quarter), quarter)
    e_keep = pl.ds(pl.multiple_of(cv * eighth, eighth), eighth)
    e_send = pl.ds(pl.multiple_of((1 - cv) * eighth, eighth), eighth)
    rows_h = pl.ds(mine, half)
    rows_send = pl.ds(pl.multiple_of(mine + (1 - cu) * quarter, quarter), quarter)
    rows_mate = [pl.ds(pl.multiple_of(theirs + c * quarter, quarter), quarter) for c in (1 - cv, cv)]
    rows_q = pl.ds(pl.multiple_of(mine + cu * quarter, quarter), quarter)
    rows_e = pl.ds(pl.multiple_of(mine + cu * quarter + cv * eighth, eighth), eighth)

    def remote(src, dst, s_sem, r_sem, to):
        return pltpu.make_async_remote_copy(
            src_ref=src, dst_ref=dst, send_sem=s_sem, recv_sem=r_sem, device_id={"dp": to}, device_id_type=MESH
        )

    part_w = width // 2

    def cols(k):
        return pl.ds(pl.multiple_of((k % per) * width, width), width)

    def cols_of(k, p):
        return pl.ds(pl.multiple_of((k % per) * width + p * part_w, part_w), part_w)

    def lanes(p):
        return pl.ds(p * part_w, part_w)

    def g_copy(s):
        return pltpu.make_async_copy(g_ref.at[0, s // per, :, cols(s)], g_buf.at[s % 2], g_sem.at[s % 2])

    def g_first(b):
        rows = pl.ds(b * rows_a, rows_a)
        return pltpu.make_async_copy(g_ref.at[0, 0, rows, pl.ds(0, width)], g_buf.at[0, rows, :], g0_sem.at[b])

    class a_copy:
        def __init__(self, b, f):
            i = b % RAW
            rows = pl.ds(pl.multiple_of((b % blocks) * rows_a, rows_a), rows_a)
            self.copies = [
                pltpu.make_async_copy(
                    a_ref.at[0, b // blocks, rows, pl.ds(pl.multiple_of(order[2 * f + c], quarter), quarter)],
                    a_raw.at[f, i, :, pl.ds(c * quarter, quarter)],
                    a_sem.at[(2 * f + c) * RAW + i],
                )
                for c in range(2)
            ]

        def start(self):
            for c in self.copies:
                c.start()

        def wait(self):
            for c in self.copies:
                c.wait()

    def d2d(s, q):
        i = s % 2
        return remote(d2d_out.at[q], d2d_in.at[i, q], d2d_s.at[q], d2d_r.at[i * 2 + q], mate)

    def rs1(k, p):
        i, j = k % SLOTS, k % SLOTS * 2 + p
        return remote(rs1_out.at[i, :, lanes(p)], rs1_in.at[i, :, lanes(p)], rs1_s.at[j], rs1_r.at[j], u)

    def rs2(k, p):
        i, j = k % SLOTS, k % SLOTS * 2 + p
        return remote(rs2_out.at[i, :, lanes(p)], rs2_in.at[i, :, lanes(p)], rs2_s.at[j], rs2_r.at[j], v)

    def gather(k, p, rows, s_sem, r_sem, to):
        j = k % HELD * 2 + p
        r = o_ref.at[k // per, rows, cols_of(k, p)]
        return remote(r, r, s_sem.at[j], r_sem.at[j], to)

    def ag1(k, p):
        return gather(k, p, rows_e, ag1_s, ag1_r, v)

    def ag2(k, p):
        return gather(k, p, rows_q, ag2_s, ag2_r, u)

    def ag3(k, p):
        return gather(k, p, rows_h, ag3_s, ag3_r, mate)

    def at(s, lag, end=steps):
        def run(f):
            k = s - lag
            pl.when(jnp.logical_and(k >= 0, k < end))(lambda: f(k))
        return run

    def gathers(s, p):
        @at(s, AG3, steps - (TAIL + p) // 2)
        def _(k):
            ag3(k, p).wait()

        @at(s, AG2, steps - (TAIL + p) // 2)
        def _(k):
            ag2(k, p).wait()
            ag3(k, p).start()

        @at(s, AG1)
        def _(k):
            ag1(k, p).wait()
            tail = 2 * (k - steps) + p + TAIL
            pl.when(tail < 0)(lambda: ag2(k, p).start())

            @pl.when(tail >= 0)
            def _():
                to = pl.ds(pl.multiple_of(tail * part_w, part_w), part_w)
                tail_ref[:, to] = o_ref[mats - 1, rows_q, cols_of(k, p)]

    def scatters(s, p):
        c = lanes(p)

        @at(s, RS2)
        def _(k):
            rs2(k, p).wait()
            i = k % SLOTS
            o_ref[k // per, rows_e, cols_of(k, p)] = (keep2[i, :, c] + rs2_in[i, :, c].astype(f32)).astype(bf16)
            ag1(k, p).start()

        @at(s, RS1)
        def _(k):
            rs1(k, p).wait()
            i = k % SLOTS
            rs2_out[i, :, c] = (keep1[i, e_send, c] + rs1_in[i, e_send, c].astype(f32)).astype(bf16)
            rs2(k, p).start()
            keep2[i, :, c] = keep1[i, e_keep, c] + rs1_in[i, e_keep, c].astype(f32)

    def events(s, p):
        gathers(s, p)
        scatters(s, p)

    def send_on(s, product):
        d2d(s, 0).wait()
        i, h = s % SLOTS, s % 2
        rs1_out[i] = (product() + d2d_in[h, 0].astype(f32)).astype(bf16)
        for p in range(2):
            rs1(s, p).start()

    def keep(s, product):
        d2d(s, 1).wait()
        i, h = s % SLOTS, s % 2
        keep1[i] = product() + d2d_in[h, 1].astype(f32)

    for b in range(RAW):
        a_copy(b, 0).start()
        g_first(b).start()

    barrier = pltpu.get_barrier_semaphore()
    for peer in (mate, u, v):
        pl.semaphore_signal(barrier, inc=1, device_id={"dp": peer}, device_id_type=MESH)

    for f in range(2):
        to = slice(2 * f * quarter, 2 * (f + 1) * quarter)
        for b in range(blocks + 1):
            if b < blocks:
                a_copy(b, f).wait()
            if b >= 1 and f == 0:
                g_first(b - 1).wait()
            if b < blocks:
                a_t[to, b * rows_a:(b + 1) * rows_a] = a_raw[f, b % RAW].T
            if b >= 1:
                k = slice((b - 1) * rows_a, b * rows_a)
                new = jnp.dot(a_t[to, k], g_buf[0, k, :], preferred_element_type=f32)
                part[to, :] = new if b == 1 else part[to, :] + new
            if b + RAW < blocks:
                a_copy(b + RAW, f).start()
                if f == 0:
                    g_first(b + RAW).start()
            elif b < blocks:
                if f == 0:
                    a_copy(b + RAW - blocks, 1).start()
                else:
                    a_copy(b + RAW, 0).start()
                    a_copy(b + RAW, 1).start()
            if f == 1 and b == blocks // 2:
                g_copy(1).start()
                send_on(0, lambda: part[send_mine, :])
        if f == 0:
            pl.semaphore_wait(barrier, 3)
        d2d_out[f] = part[(send_theirs, keep_theirs)[f], :].astype(bf16)
        d2d(0, f).start()

    @pl.loop(1, steps)
    def _(s):
        @pl.when(s % per == 0)
        def _():
            @pl.loop(s // per * blocks, s // per * blocks + blocks)
            def _(b):
                for f in range(2):
                    a_copy(b, f).wait()
                    blk = pl.ds(pl.multiple_of((b % blocks) * rows_a, rows_a), rows_a)
                    a_t[2 * f * quarter:2 * (f + 1) * quarter, blk] = a_raw[f, b % RAW].T
                    pl.when(b + RAW < mats * blocks)(lambda: a_copy(b + RAW, f).start())

        g_copy(s).wait()
        pl.when(s + 1 < steps)(lambda: g_copy(s + 1).start())
        def product(rows):
            return jnp.dot(a_t[rows, :], g_buf[s % 2], preferred_element_type=f32)

        d2d_out[0] = product(send_theirs).astype(bf16)
        d2d(s, 0).start()
        pl.when(s == 1)(lambda: keep(0, lambda: part[keep_mine, :]))
        d2d_out[1] = product(keep_theirs).astype(bf16)
        d2d(s, 1).start()
        events(s, 0)
        send_on(s, lambda: product(send_mine))
        pl.when(s <= EARLY)(lambda: events(s, 1))
        keep(s, lambda: product(keep_mine))
        pl.when(s > EARLY)(lambda: events(s, 1))

    @pl.loop(steps, steps + AG3 + 1)
    def _(s):
        scatters(s, 0)
        scatters(s, 1)
        gathers(s, 0)
        gathers(s, 1)


def place(me, d):
    half, quarter = d // 2, d // 4
    core, y, x = me % 2, (me // 2) % 2, (me // 4) % 2
    cu, cv = x + core * (y - x), y + core * (x - y)
    starts = (
        core * half + cu * quarter, core * half + (1 - cu) * quarter,
        (1 - core) * half + cv * quarter, (1 - core) * half + (1 - cv) * quarter,
    )
    return [pl.ds(pl.multiple_of(i, quarter), quarter) for i in starts]


def run(copies):
    for c in copies:
        c.start()
    for c in copies:
        c.wait()


def spread(held, o_ref, sem):
    mats, d, ff = o_ref.shape
    parts = [(n, pl.ds(i * (d // 4), d // 4)) for n in range(mats - 1) for i in range(4)]
    run([pltpu.make_async_copy(held.at[p], o_ref.at[p], sem.at[i]) for i, p in enumerate(parts)])


def spread_last(tail, held, _, o_ref, sem):
    mats, d, ff = o_ref.shape
    own = place(lax.axis_index("dp"), d)[0]
    parts = [(mats - 1, pl.ds(i * (d // 4), d // 4), pl.ds(0, ff - tail)) for i in range(4)]
    parts += [(mats - 1, own, pl.ds(ff - tail, tail))]
    run([pltpu.make_async_copy(held.at[p], o_ref.at[p], sem.at[i]) for i, p in enumerate(parts)])


def finish(from_u, from_mate, from_far, _, o_ref, sem):
    mats, d, ff = o_ref.shape
    tail = from_u.shape[1]
    rows = place(lax.axis_index("dp"), d)[1:]
    run([
        pltpu.make_async_copy(piece, o_ref.at[mats - 1, r, pl.ds(ff - tail, tail)], sem.at[i])
        for i, (piece, r) in enumerate(zip((from_u, from_mate, from_far), rows))
    ])


def solution(mesh):
    def step(a, g):
        _, mats, tokens, d = a.shape
        ff = g.shape[-1]
        width = 512 if ff % 512 == 0 else ff
        blocks = ff // width
        half, quarter, eighth = d // 2, d // 4, d // 8
        f32, bf16 = jnp.float32, jnp.bfloat16
        dma = pltpu.SemaphoreType.DMA
        tail = TAIL * width // 2
        held, quarters = pl.pallas_call(
            functools.partial(kernel, (mats, tokens, d, ff, width, blocks)),
            out_shape=(pltpu.VMEM((mats, d, ff), bf16), pltpu.VMEM((quarter, tail), bf16)),
            in_specs=[pl.BlockSpec(memory_space=pl.ANY)] * 2,
            out_specs=(pl.BlockSpec(memory_space=pltpu.VMEM), pl.BlockSpec(memory_space=pltpu.VMEM)),
            scratch_shapes=[
                pltpu.VMEM((2, RAW, tokens // blocks, half), bf16),
                pltpu.VMEM((d, tokens), bf16),
                pltpu.VMEM((2, tokens, width), bf16),
                pltpu.VMEM((2, quarter, width), bf16),
                pltpu.VMEM((2, 2, quarter, width), bf16),
                pltpu.VMEM((d, width), f32),
                pltpu.VMEM((SLOTS, quarter, width), f32),
                pltpu.VMEM((SLOTS, quarter, width), bf16),
                pltpu.VMEM((SLOTS, quarter, width), bf16),
                pltpu.VMEM((SLOTS, eighth, width), f32),
                pltpu.VMEM((SLOTS, eighth, width), bf16),
                pltpu.VMEM((SLOTS, eighth, width), bf16),
                dma((4 * RAW,)), dma((2,)), dma((blocks,)), dma((2,)), dma((4,)),
                *[dma((2 * SLOTS,)) for _ in range(4)], *[dma((2 * HELD,)) for _ in range(6)],
            ],
            compiler_params=pltpu.CompilerParams(
                collective_id=0, has_side_effects=True, vmem_limit_bytes=31 * 2**20
            ),
        )(a, g)
        devices = range(mesh.shape["dp"])
        send = lambda x, to: lax.ppermute(x, "dp", [(i, to[i]) for i in devices])
        mates = [flip(i, 1) for i in devices]
        from_u = send(quarters, [flip(i, 2 if i % 2 else 4) for i in devices])
        from_mate = send(quarters, mates)
        from_far = send(from_u, mates)
        whole = jax.ShapeDtypeStruct((mats, d, ff), bf16)
        cost = lambda n: pl.CostEstimate(flops=n * 10**10, bytes_accessed=2 * n * d * ff * 2, transcendentals=0)
        out = pl.pallas_call(
            spread,
            out_shape=whole,
            in_specs=[pl.BlockSpec(memory_space=pltpu.VMEM)],
            out_specs=pl.BlockSpec(memory_space=pl.ANY),
            scratch_shapes=[dma((4 * mats,))],
            compiler_params=pltpu.CompilerParams(vmem_limit_bytes=2**20),
            cost_estimate=cost(mats - 1),
        )(held)
        out = pl.pallas_call(
            functools.partial(spread_last, tail),
            out_shape=whole,
            in_specs=[pl.BlockSpec(memory_space=pltpu.VMEM), pl.BlockSpec(memory_space=pl.ANY)],
            out_specs=pl.BlockSpec(memory_space=pl.ANY),
            scratch_shapes=[dma((5,))],
            input_output_aliases={1: 0},
            compiler_params=pltpu.CompilerParams(vmem_limit_bytes=2**20),
            cost_estimate=cost(1),
        )(held, out)
        return pl.pallas_call(
            finish,
            out_shape=whole,
            in_specs=[pl.BlockSpec(memory_space=pltpu.VMEM)] * 3 + [pl.BlockSpec(memory_space=pl.ANY)],
            out_specs=pl.BlockSpec(memory_space=pl.ANY),
            scratch_shapes=[dma((3,))],
            input_output_aliases={3: 0},
            compiler_params=pltpu.CompilerParams(vmem_limit_bytes=8 * 2**20),
        )(from_u, from_mate, from_far, out)

    spec = P(("rep", "dp"), None, None, None)
    return jax.shard_map(step, mesh=mesh, in_specs=(spec, spec), out_specs=P("rep", None, None), check_vma=False)
```
